256 devices in a mesh: groups: 4 (over x, y), ep: 32 (over z), node: 2 (over core).
Axes of the slice: x: 2, y: 2, z: 32, core: 2. Of those that a mesh axis runs over, the one named last changes fastest.
The devices are a block of a 4x8x32 slice.
Arguments:
- tokens: bfloat16 [8192, 7168], P(('groups', 'ep', 'node')), parts along dimension 0, may hold values from -6 to 6
- expert_ids: int32 [8192, 8], P(('groups', 'ep', 'node')), parts along dimension 0, may hold values from 0 to 63, all different within a row; in each aligned block of 32 rows (0 to 31, 32 to 63, ...) at most 8 rows name the same one
- gate_weights: float32 [8192, 8], P(('groups', 'ep', 'node')), parts along dimension 0, may hold values from 0.05 to 0.5
- gate_up_weight: bfloat16 [64, 7168, 512], P(('ep', 'node')), may hold values from -0.0625 to 0.0625
- down_weight: bfloat16 [64, 256, 7168], P(('ep', 'node')), may hold values from -0.375 to 0.375
Outputs:
- moe_out: bfloat16 [8192, 7168], P(('groups', 'ep', 'node')), parts along dimension 0
The draws below stay inside these ranges and needn't reach their ends.
There are 4 independent parts, one for each index of `groups`. The reference program is written for one: setup_inputs(seed, part) draws one part's arguments, and reference() takes and returns one part's arrays. A program takes and returns all parts, laid end to end along the dimension named above; an argument that names none is the same for every part. Nothing has to cross between parts.
Inputs may be any that keep to these rules, and one draw needn't show every extreme that they name: `expert_ids`: each token names 8 different experts; among the 32 tokens of one device no expert is named by more than 8 of them, a bound that some block reaches.
All inputs are finite; a program needn't handle non-finite values.
Results may differ from the reference program's by a relative error of at most 0.0058.
Values may be sent and summed in bfloat16 or wider, within the bound.
A program may use at most 128 MiB of HBM per device.

```python
import math
import jax
import jax.numpy as jnp
import numpy as np
from jax import lax

D = 7168
TOP = 8
EXP_HID = 256
TOK_DEV = 32
EXPERTS = 64
CAP = 8
TOKENS = 2048
N_EP = 32
N_NODE = 2


def level_of(rng, dims, split, smallest, high):
    level = 1.0
    for axis_at, blocks in split:
        heights = jax.random.uniform(jax.random.fold_in(jax.random.fold_in(rng, 6), axis_at), (blocks,), jnp.float32, smallest / len(split), high / len(split))
        level = level * jnp.repeat(jnp.exp(heights), dims[axis_at] // blocks).reshape((-1,) + (1,) * (len(dims) - 1 - axis_at))
    return level


def assign_block(rng, own, number, rows, count, top, most, slope):
    sequence = jax.random.permutation(rng, count)
    heavy_load, common = load_shares(count, rows * top, most, slope, True), load_shares(count, rows * top, most, slope, False)
    places = jnp.arange(count)

    def named(sizes, turn):
        used = int((sizes > 0).sum())
        fixed = max(1, used // 4)
        shifted = fixed + (places - fixed + turn * (used - fixed)) % max(1, count - fixed)
        return jnp.zeros((count,), jnp.int32).at[sequence[jnp.where(places < fixed, places, shifted)]].set(jnp.asarray(sizes, jnp.int32))

    sizes = jnp.where(number % 4 == 0, named(heavy_load, number // 4), named(common, number - number // 4 - 1))
    mixed = jax.random.permutation(jax.random.fold_in(own, 3), count)
    source_of, taker = mixed[0:count // 2 * 2:2], mixed[1:count // 2 * 2:2]
    room = jnp.minimum(sizes[source_of] - 1, most - sizes[taker]) // 2
    room = jnp.where((source_of == sequence[0]) | (taker == sequence[0]) | (sizes[taker] == 0), 0, jnp.maximum(room, 0))
    shifted = jax.random.randint(jax.random.fold_in(own, 4), (count // 2,), 0, 1 << 20) % (room + 1)
    sizes = sizes.at[source_of].add(-shifted).at[taker].add(shifted)
    members = jnp.searchsorted(jnp.cumsum(sizes), jnp.arange(rows * top), side="right").astype(jnp.int32)
    table = members.reshape(top, rows).T
    table = table[jax.random.permutation(jax.random.fold_in(own, 1), rows)]
    turn = jax.random.randint(jax.random.fold_in(own, 2), (rows, 1), 0, top)
    return jnp.take_along_axis(table, (jnp.arange(top)[None, :] + turn) % top, axis=1)


def load_shares(amount, total, reach, skew, full):
    weights = [(1 << 20) // math.isqrt(grade ** skew) + 1 for grade in range(1, amount + 1)]
    largest = reach if full else min(reach, max(-(-total // amount), total * weights[0] // sum(weights)))
    least = 1 if total - largest >= amount - 1 else 0
    given, rest = [largest] + [least] * (amount - 1), total - largest - least * (amount - 1)
    while rest > 0:
        free = [i for i in range(1, amount) if given[i] < largest] or [i for i in range(1, amount) if given[i] < reach]
        pool, left = sum([weights[i] for i in free]), rest
        for i in free:
            extra = min(reach - given[i], max(1, left * weights[i] // pool), rest)
            given[i] = given[i] + extra
            rest = rest - extra
    return np.array(given)


def normal_values(key, extent, spread, reach, cuts=(), held_as=jnp.bfloat16):
    drawn = spread * jax.random.normal(key, extent, jnp.float32)
    if cuts:
        drawn = drawn * level_of(key, extent, cuts, -0.22, 0.18)
    return jnp.clip(drawn, -reach, reach).astype(held_as)


def setup_inputs(seed: int = 0, part: int = 0) -> dict:
    splits = jax.random.split(jax.random.key(seed), 6)
    part_keys = jax.random.split(jax.random.fold_in(splits[5], part), 6)
    tokens = normal_values(part_keys[0], (TOKENS, D), 1.0, 6.0, ((0, 64),))
    expert_ids_keys = jax.random.split(jax.random.fold_in(part_keys[1], 1), TOKENS // TOK_DEV)
    expert_ids_turns = jax.random.permutation(jax.random.fold_in(part_keys[1], 3), TOKENS // TOK_DEV)
    expert_ids = jax.vmap(lambda own, number: assign_block(jax.random.fold_in(part_keys[1], 2), own, number, TOK_DEV, EXPERTS, TOP, CAP, 2))(expert_ids_keys, expert_ids_turns).reshape((TOKENS, TOP))
    gate_weights = jnp.clip(jnp.exp(math.log(0.5) - 2.3025851 * jax.random.uniform(part_keys[2], (TOKENS, TOP), jnp.float32) ** level_of(part_keys[2], (TOKENS, TOP), ((0, 64),), -0.2, 0.2)), 0.05, 0.5)
    gate_up_weight = normal_values(splits[3], (EXPERTS, D, 2 * EXP_HID), D ** -0.5, 0.0625, ((0, 64),))
    down_weight = normal_values(splits[4], (EXPERTS, EXP_HID, D), EXP_HID ** -0.5, 0.375, ((0, 64),))
    return {"tokens": tokens, "expert_ids": expert_ids, "gate_weights": gate_weights, "gate_up_weight": gate_up_weight, "down_weight": down_weight}


def reference(tokens, expert_ids, gate_weights, gate_up_weight, down_weight):
    slot_total = N_EP * N_NODE * CAP
    token_index = jnp.arange(TOKENS, dtype=jnp.int32)

    def per_expert(running, expert):
        chosen = expert_ids == expert
        routed = jnp.any(chosen, axis=1)
        picked = jnp.sum(jnp.where(chosen, gate_weights, jnp.zeros_like(gate_weights)), axis=1)
        position = jnp.cumsum(routed.astype(jnp.int32)) - 1
        where_to = jnp.where(routed, position, slot_total).astype(jnp.int32)
        row_index = jnp.zeros((slot_total,), jnp.int32).at[where_to].set(token_index, mode="drop")
        filled = jnp.zeros((slot_total,), jnp.float32).at[where_to].set(jnp.ones((TOKENS,), jnp.float32), mode="drop")
        gathered = tokens[row_index]
        gate_up = jnp.dot(gathered, gate_up_weight[expert], preferred_element_type=jnp.float32)
        hidden = (jax.nn.silu(gate_up[:, :EXP_HID]) * gate_up[:, EXP_HID:]).astype(jnp.bfloat16)
        result = jnp.dot(hidden, down_weight[expert], preferred_element_type=jnp.float32).astype(jnp.bfloat16)
        weight_row = filled * picked[row_index]
        running = running.at[row_index].add(weight_row[:, None] * result.astype(jnp.float32))
        return running, None

    start = jnp.zeros((TOKENS, D), jnp.float32)
    summed, unused = lax.scan(per_expert, start, jnp.arange(EXPERTS, dtype=jnp.int32))
    return summed.astype(jnp.bfloat16)
```

```python
import functools

import jax
import jax.numpy as jnp
from jax import lax
from jax.experimental import pallas as pl
from jax.experimental.pallas import tpu as pltpu
from jax.sharding import PartitionSpec as P

MESH = pl.DeviceIdType.MESH
BF16 = jnp.bfloat16
F32 = jnp.float32
LEFT, RIGHT = 0, 1


def moe_kernel(
    n, nch, top,
    tok_hbm, meta_in, gu_hbm, dn_hbm, out_ref,
    tok, meta, wgu, wd, hid, acc, part,
    load_sem, w_send, w_recv, ag_send, ag_recv, meta_send, meta_recv, rs_send, rs_recv,
):
    half = n // 2
    hch = nch // 2
    rows, width = tok.shape[2], tok.shape[3]
    inner = dn_hbm.shape[1]
    me = lax.axis_index("ep")
    core = lax.axis_index("node")
    right, left = lax.rem(me + 1, n), lax.rem(me + n - 1, n)
    peer = 1 - core

    barrier = pltpu.get_barrier_semaphore()
    pl.semaphore_signal(barrier, inc=1, device_id={"ep": left}, device_id_type=MESH)
    pl.semaphore_signal(barrier, inc=1, device_id={"ep": right}, device_id_type=MESH)
    pl.semaphore_signal(barrier, inc=1, device_id={"node": peer}, device_id_type=MESH)

    loads = []
    for j in range(nch):
        loads.append(pltpu.make_async_copy(
            tok_hbm.at[:, pl.ds(j * width, width)], tok.at[0, j], load_sem.at[j]))
    loads.append(pltpu.make_async_copy(meta_in, meta.at[0], load_sem.at[nch]))
    for c in loads:
        c.start()
    w_loads = [pltpu.make_async_copy(gu_hbm.at[0], wgu.at[0], load_sem.at[nch + 1])]
    w_remote = [pltpu.make_async_remote_copy(
        src_ref=gu_hbm.at[0], dst_ref=wgu.at[1], send_sem=w_send.at[0], recv_sem=w_recv.at[0],
        device_id={"node": peer}, device_id_type=MESH)]
    for j in range(nch):
        src = dn_hbm.at[0, :, pl.ds(j * width, width)]
        w_loads.append(pltpu.make_async_copy(
            src, wd.at[j, pl.ds(0, inner)], load_sem.at[nch + 2 + j]))
        w_remote.append(pltpu.make_async_remote_copy(
            src_ref=src, dst_ref=wd.at[j, pl.ds(inner, inner)],
            send_sem=w_send.at[1 + j], recv_sem=w_recv.at[1 + j],
            device_id={"node": peer}, device_id_type=MESH))
    for c in loads:
        c.wait()
    for c in w_loads:
        c.start()
    pl.semaphore_wait(barrier, 3)

    def slots(direction, s):
        return lax.rem(n - s, n) if direction == LEFT else s

    def ag(direction, s, j):
        return pltpu.make_async_remote_copy(
            src_ref=tok.at[slots(direction, s - 1), j], dst_ref=tok.at[slots(direction, s), j],
            send_sem=ag_send.at[direction, j], recv_sem=ag_recv.at[direction, s, j],
            device_id={"ep": left if direction == LEFT else right}, device_id_type=MESH)

    def ag_meta(direction, s):
        return pltpu.make_async_remote_copy(
            src_ref=meta.at[slots(direction, s - 1)], dst_ref=meta.at[slots(direction, s)],
            send_sem=meta_send.at[direction], recv_sem=meta_recv.at[direction, s],
            device_id={"ep": left if direction == LEFT else right}, device_id_type=MESH)

    def rs(direction, d, j):
        return pltpu.make_async_remote_copy(
            src_ref=part.at[direction, d, j], dst_ref=part.at[direction, d - 1, j],
            send_sem=rs_send.at[direction, j], recv_sem=rs_recv.at[direction, d - 1, j],
            device_id={"ep": left if direction == LEFT else right}, device_id_type=MESH)

    def rs_arrive(direction, d, j):
        return rs(direction, d + 1, j)

    def loop(lo, hi, body):
        def step(i, carry):
            body(i)
            return carry
        lax.fori_loop(lo, hi, step, 0)

    def matmul(a, b, j):
        x = jnp.concatenate([tok[a, j], tok[b, j]], axis=0)
        for e in range(2):
            at = pl.ds(e * 2 * inner, 2 * inner)
            w = wgu[e, pl.ds(pl.multiple_of(j * width, width), width), :]
            acc[:, at] += jnp.dot(x, w, preferred_element_type=F32)

    same = (lax.broadcasted_iota(jnp.int32, (rows, 128), 0)
            == lax.broadcasted_iota(jnp.int32, (rows, 128), 1))

    def gate_column(slot, expert):
        ids = meta[slot]
        gates = pltpu.roll(ids, 128 - rows, 1)
        row = jnp.sum(jnp.where(ids == expert, gates, 0.0), axis=0, keepdims=True)
        return jnp.sum(jnp.where(same, row, 0.0), axis=1, keepdims=True)

    def activate(a, b):
        for e, owner in ((0, core), (1, peer)):
            expert = (me * 2 + owner).astype(F32)
            g = jnp.concatenate([gate_column(a, expert), gate_column(b, expert)], axis=0)
            gate = acc[:, pl.ds(e * 2 * inner, inner)]
            up = acc[:, pl.ds(e * 2 * inner + inner, inner)]
            h = (gate * (1.0 / (1.0 + jnp.exp(-gate))) * up * g).astype(BF16)
            hid[a, :, pl.ds(e * inner, inner)] = h[:rows]
            hid[b, :, pl.ds(e * inner, inner)] = h[rows:]
        acc[...] = jnp.zeros_like(acc)

    for j in range(nch):
        for direction in (LEFT, RIGHT):
            ag(direction, 1, j).start()
    for direction in (LEFT, RIGHT):
        ag_meta(direction, 1).start()
    for c in w_remote:
        c.start()
    acc[...] = jnp.zeros_like(acc)

    def pass_on(s, j, directions):
        for direction in (LEFT, RIGHT):
            arrived = ag(direction, s, j)
            arrived.wait_recv()
            arrived.wait_send()
            if direction in directions:
                ag(direction, s + 1, j).start()

    def pass_meta(s, directions):
        for direction in (LEFT, RIGHT):
            arrived = ag_meta(direction, s)
            arrived.wait_recv()
            arrived.wait_send()
            if direction in directions:
                ag_meta(direction, s + 1).start()

    loop(0, nch, lambda j: pass_on(1, j, (LEFT, RIGHT)))
    pass_meta(1, (LEFT, RIGHT))
    w_loads[0].wait()
    w_remote[0].wait_recv()

    def gather_step(s):
        def chunk(j):
            pass_on(s, j, (LEFT, RIGHT))
            matmul(s - 1, n - s + 1, j)
        loop(0, nch, chunk)
        pass_meta(s, (LEFT, RIGHT))
        activate(s - 1, n - s + 1)

    loop(2, half - 1, gather_step)

    def last_right(j):
        pass_on(half - 1, j, (RIGHT,))
        matmul(half - 2, half + 2, j)

    def last_left(j):
        pass_on(half - 1, j, (LEFT,))
        matmul(half - 2, half + 2, j)

    loop(0, hch, last_right)
    loop(hch, nch, last_left)
    pass_meta(half - 1, (RIGHT,))
    activate(half - 2, half + 2)

    loop(0, nch, lambda j: matmul(half - 1, half + 1, j))
    activate(half - 1, half + 1)

    for c in w_loads[1:]:
        c.wait()
    for c in w_remote[1:]:
        c.wait_recv()

    def pair(d, j):
        h = jnp.concatenate([hid[d], hid[n - d]], axis=0)
        return jnp.dot(h, wd[j], preferred_element_type=F32)

    def free_chunk(direction):
        def body(j):
            h = hid[half - 1] if direction == LEFT else hid[half + 1]
            part[direction, half - 1, j] = jnp.dot(
                h, wd[j], preferred_element_type=F32).astype(BF16)
            rs(direction, half - 1, j).start()
        return body

    loop(hch, nch, free_chunk(LEFT))
    loop(0, hch, free_chunk(RIGHT))

    def far(direction):
        def body(j):
            ag(direction, half, j).wait_recv()
            ag(direction, half, j).wait_send()
            matmul(half, 0, j)
        return body

    loop(0, hch, far(RIGHT))
    loop(hch, nch, far(LEFT))
    ag_meta(RIGHT, half).wait()
    activate(half, 0)

    def far_chunk(direction):
        def body(j):
            part[direction, half, j] = jnp.dot(
                hid[half], wd[j], preferred_element_type=F32).astype(BF16)
            rs(direction, half, j).start()
        return body

    loop(0, hch, far_chunk(LEFT))
    loop(hch, nch, far_chunk(RIGHT))

    def second_chunk(direction):
        def body(j):
            h = hid[half - 1] if direction == LEFT else hid[half + 1]
            mine = jnp.dot(h, wd[j], preferred_element_type=F32)
            rs_arrive(direction, half - 1, j).wait_recv()
            total = mine + part[direction, half - 1, j].astype(F32)
            part[direction, half - 1, j] = total.astype(BF16)
            rs(direction, half, j).wait_send()
            rs(direction, half - 1, j).start()
        return body

    loop(0, hch, second_chunk(LEFT))
    loop(hch, nch, second_chunk(RIGHT))

    def reduce_step(i):
        d = half - 2 - i

        def chunk(j):
            mine = pair(d, j)
            for direction in (LEFT, RIGHT):
                rs_arrive(direction, d, j).wait_recv()
                own = mine[:rows] if direction == LEFT else mine[rows:]
                total = own + part[direction, d, j].astype(F32)
                part[direction, d, j] = total.astype(BF16)
                rs(direction, d + 1, j).wait_send()
            for direction in (LEFT, RIGHT):
                rs(direction, d, j).start()
        loop(0, nch, chunk)

    loop(0, half - 2, reduce_step)

    for j in range(nch):
        total = jnp.dot(hid[0], wd[j], preferred_element_type=F32)
        for direction in (LEFT, RIGHT):
            rs_arrive(direction, 0, j).wait()
            total = total + part[direction, 0, j].astype(F32)
        out_ref[:, pl.ds(j * width, width)] = total.astype(BF16)
    for c in w_remote:
        c.wait_send()


def on_device(n, tokens, expert_ids, gate_weights, gate_up_weight, down_weight):
    rows, model = tokens.shape
    top = expert_ids.shape[1]
    inner = down_weight.shape[1]
    nch = 4
    width = model // nch
    half = n // 2
    meta = jnp.concatenate(
        [expert_ids.T.astype(F32), gate_weights.T, jnp.zeros((top, 128 - 2 * rows), F32)], axis=1)
    dma = pltpu.SemaphoreType.DMA
    hbm = pl.BlockSpec(memory_space=pl.ANY)
    vmem = pl.BlockSpec(memory_space=pltpu.VMEM)
    return pl.pallas_call(
        functools.partial(moe_kernel, n, nch, top),
        out_shape=jax.ShapeDtypeStruct((rows, model), BF16),
        in_specs=[hbm, vmem, hbm, hbm],
        out_specs=vmem,
        scratch_shapes=[
            pltpu.VMEM((n, nch, rows, width), BF16),
            pltpu.VMEM((n, top, 128), F32),
            pltpu.VMEM((2, model, 2 * inner), BF16),
            pltpu.VMEM((nch, 2 * inner, width), BF16),
            pltpu.VMEM((n, rows, 2 * inner), BF16),
            pltpu.VMEM((2 * rows, 4 * inner), F32),
            pltpu.VMEM((2, half + 1, nch, rows, width), BF16),
            dma((2 * nch + 2,)),
            dma((1 + nch,)),
            dma((1 + nch,)),
            dma((2, nch)),
            dma((2, half + 1, nch)),
            dma((2,)),
            dma((2, half + 1)),
            dma((2, nch)),
            dma((2, half + 1, nch)),
        ],
        compiler_params=pltpu.CompilerParams(
            collective_id=0, has_side_effects=True, vmem_limit_bytes=66_000_000),
        name="moe_ring",
    )(tokens, meta, gate_up_weight, down_weight)


def solution(mesh):
    placed = (
        P(("groups", "ep", "node"), None),
        P(("groups", "ep", "node"), None),
        P(("groups", "ep", "node"), None),
        P(("ep", "node"), None, None),
        P(("ep", "node"), None, None),
    )
    return jax.shard_map(
        functools.partial(on_device, mesh.shape["ep"]),
        mesh=mesh,
        in_specs=placed,
        out_specs=P(("groups", "ep", "node"), None),
        check_vma=False,
    )
```

```python
import functools

import jax
import jax.numpy as jnp
from jax import lax
from jax.experimental import pallas as pl
from jax.experimental.pallas import tpu as pltpu
from jax.sharding import PartitionSpec as P

MESH = pl.DeviceIdType.MESH
BF16 = jnp.bfloat16
F32 = jnp.float32
LEFT, RIGHT = 0, 1


def moe_kernel(
    n, nch, top,
    tok_hbm, ids_hbm, gates_hbm, gu_hbm, dn_hbm, out_hbm,
    tok, ids_in, gates_in, meta, wgu, wd, hid, acc, part, out_buf,
    load_sem, out_sem, w_send, w_recv, ag_send, ag_recv, meta_send, meta_recv, rs_send, rs_recv,
):
    half = n // 2
    hch = nch // 2
    rows, width = tok.shape[2], tok.shape[3]
    inner = dn_hbm.shape[1]
    me = lax.axis_index("ep")
    core = lax.axis_index("node")
    right, left = lax.rem(me + 1, n), lax.rem(me + n - 1, n)
    peer = 1 - core

    barrier = pltpu.get_barrier_semaphore()
    pl.semaphore_signal(barrier, inc=1, device_id={"ep": left}, device_id_type=MESH)
    pl.semaphore_signal(barrier, inc=1, device_id={"ep": right}, device_id_type=MESH)
    pl.semaphore_signal(barrier, inc=1, device_id={"node": peer}, device_id_type=MESH)

    tok_loads = [pltpu.make_async_copy(
        tok_hbm.at[:, pl.ds(j * width, width)], tok.at[0, j], load_sem.at[j]) for j in range(nch)]
    meta_loads = [
        pltpu.make_async_copy(ids_hbm, ids_in, load_sem.at[nch]),
        pltpu.make_async_copy(gates_hbm, gates_in, load_sem.at[nch + 1]),
    ]
    for c in tok_loads + meta_loads:
        c.start()

    def gu_load(j):
        at = pl.ds(j * width, width)
        return pltpu.make_async_copy(gu_hbm.at[0, at], wgu.at[0, at], load_sem.at[nch + 2 + j])

    def gu_swap(j):
        at = pl.ds(j * width, width)
        return pltpu.make_async_remote_copy(
            src_ref=gu_hbm.at[0, at], dst_ref=wgu.at[1, at],
            send_sem=w_send.at[j], recv_sem=w_recv.at[j],
            device_id={"node": peer}, device_id_type=MESH)

    def dn_load(j):
        return pltpu.make_async_copy(
            dn_hbm.at[0, :, pl.ds(j * width, width)], wd.at[j, pl.ds(0, inner)],
            load_sem.at[2 * nch + 2 + j])

    def dn_swap(j):
        return pltpu.make_async_remote_copy(
            src_ref=dn_hbm.at[0, :, pl.ds(j * width, width)], dst_ref=wd.at[j, pl.ds(inner, inner)],
            send_sem=w_send.at[nch + j], recv_sem=w_recv.at[nch + j],
            device_id={"node": peer}, device_id_type=MESH)

    for c in meta_loads:
        c.wait()
    meta[0] = jnp.concatenate(
        [ids_in[...].astype(F32), gates_in[...], jnp.zeros((top, 128 - 2 * rows), F32)], axis=1)
    pl.semaphore_wait(barrier, 3)

    def slots(direction, s):
        return lax.rem(n - s, n) if direction == LEFT else s

    def ag(direction, s, j):
        return pltpu.make_async_remote_copy(
            src_ref=tok.at[slots(direction, s - 1), j], dst_ref=tok.at[slots(direction, s), j],
            send_sem=ag_send.at[direction, j], recv_sem=ag_recv.at[direction, s, j],
            device_id={"ep": left if direction == LEFT else right}, device_id_type=MESH)

    def ag_meta(direction, s):
        return pltpu.make_async_remote_copy(
            src_ref=meta.at[slots(direction, s - 1)], dst_ref=meta.at[slots(direction, s)],
            send_sem=meta_send.at[direction], recv_sem=meta_recv.at[direction, s],
            device_id={"ep": left if direction == LEFT else right}, device_id_type=MESH)

    def rs(direction, d, j):
        return pltpu.make_async_remote_copy(
            src_ref=part.at[direction, d, j], dst_ref=part.at[direction, d - 1, j],
            send_sem=rs_send.at[direction, j], recv_sem=rs_recv.at[direction, d - 1, j],
            device_id={"ep": left if direction == LEFT else right}, device_id_type=MESH)

    def rs_arrive(direction, d, j):
        return rs(direction, d + 1, j)

    def loop(lo, hi, body):
        def step(i, carry):
            body(i)
            return carry
        lax.fori_loop(lo, hi, step, 0)

    def matmul(blocks, j):
        x = jnp.concatenate([tok[a, j] for a in blocks], axis=0)
        for e in range(2):
            at = pl.ds(e * 2 * inner, 2 * inner)
            w = wgu[e, pl.ds(pl.multiple_of(j * width, width), width), :]
            acc[: len(blocks) * rows, at] += jnp.dot(x, w, preferred_element_type=F32)

    same = (lax.broadcasted_iota(jnp.int32, (rows, 128), 0)
            == lax.broadcasted_iota(jnp.int32, (rows, 128), 1))

    def gate_column(slot, expert):
        ids = meta[slot]
        gates = pltpu.roll(ids, 128 - rows, 1)
        row = jnp.sum(jnp.where(ids == expert, gates, 0.0), axis=0, keepdims=True)
        return jnp.sum(jnp.where(same, row, 0.0), axis=1, keepdims=True)

    def activate(blocks):
        count = len(blocks) * rows
        for e, owner in ((0, core), (1, peer)):
            expert = (me * 2 + owner).astype(F32)
            g = jnp.concatenate([gate_column(a, expert) for a in blocks], axis=0)
            gate = acc[:count, pl.ds(e * 2 * inner, inner)]
            up = acc[:count, pl.ds(e * 2 * inner + inner, inner)]
            h = (gate * (1.0 / (1.0 + jnp.exp(-gate))) * up * g).astype(BF16)
            for i, a in enumerate(blocks):
                hid[a, :, pl.ds(e * inner, inner)] = h[i * rows:(i + 1) * rows]
        acc[:count, :] = jnp.zeros((count, 4 * inner), F32)

    for j in range(nch):
        tok_loads[j].wait()
        for direction in (LEFT, RIGHT):
            ag(direction, 1, j).start()
    for direction in (LEFT, RIGHT):
        ag_meta(direction, 1).start()
    for j in range(nch):
        gu_load(j).start()
        gu_swap(j).start()
    acc[...] = jnp.zeros_like(acc)

    def pass_on(s, j, directions):
        for direction in (LEFT, RIGHT):
            arrived = ag(direction, s, j)
            arrived.wait_recv()
            arrived.wait_send()
            if direction in directions:
                ag(direction, s + 1, j).start()

    def pass_meta(s, directions):
        for direction in (LEFT, RIGHT):
            arrived = ag_meta(direction, s)
            arrived.wait_recv()
            arrived.wait_send()
            if direction in directions:
                ag_meta(direction, s + 1).start()

    loop(0, nch, lambda j: pass_on(1, j, (LEFT, RIGHT)))
    pass_meta(1, (LEFT, RIGHT))

    def first_chunks(j):
        pass_on(2, j, (LEFT, RIGHT))
        gu_load(j).wait()
        gu_swap(j).wait_recv()
        dn_load(j).start()
        dn_swap(j).start()
        matmul((0, 1, n - 1, 2, n - 2), j)

    loop(0, nch, first_chunks)
    pass_meta(2, (LEFT, RIGHT))
    activate((0, 1, n - 1, 2, n - 2))

    def gather_step(s):
        def chunk(j):
            pass_on(s, j, (LEFT, RIGHT))
            matmul((s, n - s), j)
        loop(0, nch, chunk)
        pass_meta(s, (LEFT, RIGHT))
        activate((s, n - s))

    loop(3, half - 1, gather_step)

    def last_right(j):
        pass_on(half - 1, j, (RIGHT,))
        matmul((half - 1, half + 1), j)

    def last_left(j):
        pass_on(half - 1, j, (LEFT,))
        matmul((half - 1, half + 1), j)

    loop(0, hch, last_right)
    loop(hch, nch, last_left)
    pass_meta(half - 1, (RIGHT,))
    for j in range(nch):
        dn_load(j).wait()
        dn_swap(j).wait_recv()
    activate((half - 1, half + 1))

    def pair(d, j):
        h = jnp.concatenate([hid[d], hid[n - d]], axis=0)
        return jnp.dot(h, wd[j], preferred_element_type=F32)

    sides = ((LEFT, half - 1, 0), (RIGHT, half + 1, hch))

    def free_chunk(i):
        for direction, slot, first in sides:
            j = hch - first + i
            part[direction, half - 1, j] = jnp.dot(
                hid[slot], wd[j], preferred_element_type=F32).astype(BF16)
            rs(direction, half - 1, j).start()

    loop(0, hch, free_chunk)

    def far(i):
        for direction, first in ((RIGHT, 0), (LEFT, hch)):
            j = first + i
            ag(direction, half, j).wait()
            matmul((half,), j)

    loop(0, hch, far)
    ag_meta(RIGHT, half).wait()
    activate((half,))

    def far_chunk(i):
        for direction, slot, first in sides:
            j = first + i
            part[direction, half, j] = jnp.dot(
                hid[half], wd[j], preferred_element_type=F32).astype(BF16)
            rs(direction, half, j).start()

    loop(0, hch, far_chunk)

    def second_chunk(i):
        for direction, slot, first in sides:
            j = first + i
            mine = jnp.dot(hid[slot], wd[j], preferred_element_type=F32)
            rs_arrive(direction, half - 1, j).wait_recv()
            total = mine + part[direction, half - 1, j].astype(F32)
            part[direction, half - 1, j] = total.astype(BF16)
            rs(direction, half, j).wait_send()
            rs(direction, half - 1, j).start()

    loop(0, hch, second_chunk)

    def reduce_step(i):
        d = half - 2 - i

        def chunk(j):
            mine = pair(d, j)
            for direction in (LEFT, RIGHT):
                rs_arrive(direction, d, j).wait_recv()
                own = mine[:rows] if direction == LEFT else mine[rows:]
                total = own + part[direction, d, j].astype(F32)
                part[direction, d, j] = total.astype(BF16)
                rs(direction, d + 1, j).wait_send()
            for direction in (LEFT, RIGHT):
                rs(direction, d, j).start()
        loop(0, nch, chunk)

    loop(0, half - 2, reduce_step)

    def out_copy(j):
        return pltpu.make_async_copy(
            out_buf.at[j], out_hbm.at[:, pl.ds(j * width, width)], out_sem.at[j])

    for j in range(nch):
        total = jnp.dot(hid[0], wd[j], preferred_element_type=F32)
        for direction in (LEFT, RIGHT):
            rs_arrive(direction, 0, j).wait()
            total = total + part[direction, 0, j].astype(F32)
        out_buf[j] = total.astype(BF16)
        out_copy(j).start()
    for j in range(nch):
        gu_swap(j).wait_send()
        dn_swap(j).wait_send()
        out_copy(j).wait()


def on_device(n, tokens, expert_ids, gate_weights, gate_up_weight, down_weight):
    rows, model = tokens.shape
    top = expert_ids.shape[1]
    inner = down_weight.shape[1]
    nch = 4
    width = model // nch
    half = n // 2
    dma = pltpu.SemaphoreType.DMA
    hbm = pl.BlockSpec(memory_space=pl.ANY)
    return pl.pallas_call(
        functools.partial(moe_kernel, n, nch, top),
        out_shape=jax.ShapeDtypeStruct((rows, model), BF16),
        in_specs=[hbm] * 5,
        out_specs=hbm,
        scratch_shapes=[
            pltpu.VMEM((n, nch, rows, width), BF16),
            pltpu.VMEM((top, rows), jnp.int32),
            pltpu.VMEM((top, rows), F32),
            pltpu.VMEM((n, top, 128), F32),
            pltpu.VMEM((2, model, 2 * inner), BF16),
            pltpu.VMEM((nch, 2 * inner, width), BF16),
            pltpu.VMEM((n, rows, 2 * inner), BF16),
            pltpu.VMEM((5 * rows, 4 * inner), F32),
            pltpu.VMEM((2, half + 1, nch, rows, width), BF16),
            pltpu.VMEM((nch, rows, width), BF16),
            dma((3 * nch + 2,)),
            dma((nch,)),
            dma((2 * nch,)),
            dma((2 * nch,)),
            dma((2, nch)),
            dma((2, half + 1, nch)),
            dma((2,)),
            dma((2, half + 1)),
            dma((2, nch)),
            dma((2, half + 1, nch)),
        ],
        compiler_params=pltpu.CompilerParams(
            collective_id=0, has_side_effects=True, vmem_limit_bytes=66_000_000),
        name="moe_ring",
    )(tokens, expert_ids.T, gate_weights.T, gate_up_weight, down_weight)


def solution(mesh):
    placed = (
        P(("groups", "ep", "node"), None),
        P(("groups", "ep", "node"), None),
        P(("groups", "ep", "node"), None),
        P(("ep", "node"), None, None),
        P(("ep", "node"), None, None),
    )
    return jax.shard_map(
        functools.partial(on_device, mesh.shape["ep"]),
        mesh=mesh,
        in_specs=placed,
        out_specs=P(("groups", "ep", "node"), None),
        check_vma=False,
    )
```

```python
import functools

import jax
import jax.numpy as jnp
from jax import lax
from jax.experimental import pallas as pl
from jax.experimental.pallas import tpu as pltpu
from jax.sharding import PartitionSpec as P

MESH = pl.DeviceIdType.MESH
BF16 = jnp.bfloat16
F32 = jnp.float32
AHEAD, BEHIND = 0, 1


def moe_kernel(
    n, nch, top, cap,
    tok_hbm, ids_hbm, gates_hbm, gu_hbm, dn_hbm, out_hbm,
    tok, ids_in, gates_in, meta, wgu, wd, hid, hid_few, acc, part, out_buf,
    few_out, few_in, back_out, back_in,
    load_sem, out_sem, w_send, w_recv, ag_send, ag_recv, meta_send, meta_recv,
    few_send, few_recv, rs_send, rs_recv, back_send, back_recv,
):
    half = n // 2
    few = 2 * cap
    rows, width = tok.shape[2], tok.shape[3]
    inner = dn_hbm.shape[1]
    me = lax.axis_index("ep")
    core = lax.axis_index("node")
    peer = 1 - core
    ahead = lax.rem(me + 1 + core * (n - 2), n)
    behind = lax.rem(me + n - 1 - core * (n - 2), n)
    to = (ahead, behind)

    barrier = pltpu.get_barrier_semaphore()
    pl.semaphore_signal(barrier, inc=1, device_id={"ep": ahead}, device_id_type=MESH)
    pl.semaphore_signal(barrier, inc=1, device_id={"ep": behind}, device_id_type=MESH)
    pl.semaphore_signal(barrier, inc=1, device_id={"node": peer}, device_id_type=MESH)

    tok_loads = [pltpu.make_async_copy(
        tok_hbm.at[:, pl.ds(j * width, width)], tok.at[0, j], load_sem.at[j]) for j in range(nch)]
    meta_loads = [
        pltpu.make_async_copy(ids_hbm, ids_in, load_sem.at[nch]),
        pltpu.make_async_copy(gates_hbm, gates_in, load_sem.at[nch + 1]),
    ]
    for c in meta_loads + tok_loads:
        c.start()

    def gu_load(j):
        at = pl.ds(j * width, width)
        return pltpu.make_async_copy(gu_hbm.at[0, at], wgu.at[0, at], load_sem.at[nch + 2 + j])

    def gu_swap(j):
        at = pl.ds(j * width, width)
        return pltpu.make_async_remote_copy(
            src_ref=gu_hbm.at[0, at], dst_ref=wgu.at[1, at],
            send_sem=w_send.at[j], recv_sem=w_recv.at[j],
            device_id={"node": peer}, device_id_type=MESH)

    def dn_load(j):
        return pltpu.make_async_copy(
            dn_hbm.at[0, :, pl.ds(j * width, width)], wd.at[j, pl.ds(0, inner)],
            load_sem.at[2 * nch + 2 + j])

    def dn_swap(j):
        return pltpu.make_async_remote_copy(
            src_ref=dn_hbm.at[0, :, pl.ds(j * width, width)], dst_ref=wd.at[j, pl.ds(inner, inner)],
            send_sem=w_send.at[nch + j], recv_sem=w_recv.at[nch + j],
            device_id={"node": peer}, device_id_type=MESH)

    for c in meta_loads:
        c.wait()
    meta[0] = jnp.concatenate(
        [ids_in[...].astype(F32), gates_in[...], jnp.zeros((top, 128 - 2 * rows), F32)], axis=1)
    pl.semaphore_wait(barrier, 3)

    def slot(way, s):
        return s if way == AHEAD else lax.rem(n - s, n)

    def ag(way, s, j):
        return pltpu.make_async_remote_copy(
            src_ref=tok.at[slot(way, s - 1), j], dst_ref=tok.at[slot(way, s), j],
            send_sem=ag_send.at[way, j], recv_sem=ag_recv.at[way, s, j],
            device_id={"ep": to[way]}, device_id_type=MESH)

    def ag_meta(way, s):
        return pltpu.make_async_remote_copy(
            src_ref=meta.at[slot(way, s - 1)], dst_ref=meta.at[slot(way, s)],
            send_sem=meta_send.at[way], recv_sem=meta_recv.at[way, s],
            device_id={"ep": to[way]}, device_id_type=MESH)

    def ag_few(way, j):
        return pltpu.make_async_remote_copy(
            src_ref=few_out.at[way, j], dst_ref=few_in.at[way, j],
            send_sem=few_send.at[way, j], recv_sem=few_recv.at[way, j],
            device_id={"ep": to[way]}, device_id_type=MESH)

    def rs(way, d, j):
        return pltpu.make_async_remote_copy(
            src_ref=part.at[way, d, j], dst_ref=part.at[way, d - 1, j],
            send_sem=rs_send.at[way, j], recv_sem=rs_recv.at[way, d - 1, j],
            device_id={"ep": to[way]}, device_id_type=MESH)

    def rs_few(way, j):
        return pltpu.make_async_remote_copy(
            src_ref=back_out.at[way, j], dst_ref=back_in.at[way, j],
            send_sem=back_send.at[way, j], recv_sem=back_recv.at[way, j],
            device_id={"ep": to[way]}, device_id_type=MESH)

    def loop(lo, hi, body):
        def step(i, carry):
            body(i)
            return carry
        lax.fori_loop(lo, hi, step, 0)

    def matmul(x, j):
        for e in range(2):
            at = pl.ds(e * 2 * inner, 2 * inner)
            w = wgu[e, pl.ds(pl.multiple_of(j * width, width), width), :]
            acc[: x.shape[0], at] += jnp.dot(x, w, preferred_element_type=F32)

    def blocks(slots, j):
        return jnp.concatenate([tok[a, j] for a in slots], axis=0)

    lane = lax.broadcasted_iota(jnp.int32, (rows, 128), 1)
    same = lax.broadcasted_iota(jnp.int32, (rows, 128), 0) == lane
    before = (lax.broadcasted_iota(jnp.int32, (128, 128), 0)
              < lax.broadcasted_iota(jnp.int32, (128, 128), 1)).astype(F32).astype(BF16)

    def expert(chip, e):
        return (chip * 2 + (core if e == 0 else peer)).astype(F32)

    def gate_row(a, name):
        ids = meta[a]
        return jnp.sum(jnp.where(ids == name, pltpu.roll(ids, 128 - rows, 1), 0.0), axis=0, keepdims=True)

    def chosen_row(a, name):
        return jnp.sum(jnp.where(meta[a] == name, 1.0, 0.0), axis=0, keepdims=True)

    def rank_row(chosen):
        wide = jnp.broadcast_to(chosen, (8, 128)).astype(BF16)
        return jnp.dot(wide, before, preferred_element_type=F32)[0:1]

    def column(row):
        return jnp.sum(jnp.where(same, row, 0.0), axis=1, keepdims=True)

    def pick(a, chip):
        place = lax.broadcasted_iota(jnp.int32, (few, 128), 0).astype(F32)
        found = jnp.zeros((few, 128), F32)
        for e in range(2):
            chosen = chosen_row(a, expert(chip, e))
            found += jnp.where(place - e * cap == rank_row(chosen), chosen, 0.0)
        return found

    def unpick(a, chip):
        place = lane.astype(F32)
        found = jnp.zeros((rows, 128), F32)
        for e in range(2):
            chosen = chosen_row(a, expert(chip, e))
            found += jnp.where(place - e * cap == column(rank_row(chosen)), column(chosen), 0.0)
        return found[:, :few].astype(BF16)

    def gate_all(a, e):
        return column(gate_row(a, expert(me, e)))

    def gate_few(a, e):
        place = lax.broadcasted_iota(jnp.int32, (few, 128), 0).astype(F32) - e * cap
        name = expert(me, e)
        chosen = chosen_row(a, name)
        hit = jnp.where(place == rank_row(chosen), chosen * gate_row(a, name), 0.0)
        return jnp.sum(jnp.where(lax.broadcasted_iota(jnp.int32, (few, 128), 1) < rows, hit, 0.0),
                       axis=1, keepdims=True)

    def activate(slots, few_slots=()):
        count = len(slots) * rows + len(few_slots) * few
        for e in range(2):
            g = jnp.concatenate(
                [gate_all(a, e) for a in slots]
                + [gate_few(slot(way, half - way), e) for way in few_slots], axis=0)
            gate = acc[:count, pl.ds(e * 2 * inner, inner)]
            up = acc[:count, pl.ds(e * 2 * inner + inner, inner)]
            h = (gate * (1.0 / (1.0 + jnp.exp(-gate))) * up * g).astype(BF16)
            at = pl.ds(e * inner, inner)
            for i, a in enumerate(slots):
                hid[a, :, at] = h[i * rows:(i + 1) * rows]
            for i, way in enumerate(few_slots):
                first = len(slots) * rows + i * few
                hid_few[way, :, at] = h[first:first + few]
        acc[:count, :] = jnp.zeros((count, 4 * inner), F32)

    for way in (AHEAD, BEHIND):
        ag_meta(way, 1).start()
    for j in range(nch):
        tok_loads[j].wait()
        for way in (AHEAD, BEHIND):
            ag(way, 1, j).start()
    for j in range(nch):
        gu_load(j).start()
        gu_swap(j).start()
    acc[...] = jnp.zeros_like(acc)

    def arrive(copy):
        copy.wait_recv()
        copy.wait_send()

    def pass_on(s, j):
        for way in (AHEAD, BEHIND):
            arrive(ag(way, s, j))
            ag(way, s + 1, j).start()

    def pass_meta(s, ways=(AHEAD, BEHIND)):
        for way in (AHEAD, BEHIND):
            arrive(ag_meta(way, s))
            if way in ways:
                ag_meta(way, s + 1).start()

    pass_meta(1)
    loop(0, nch, lambda j: pass_on(1, j))

    opening = (0, 1, n - 1, 2, n - 2)

    def first_chunks(j):
        pass_on(2, j)
        gu_load(j).wait()
        gu_swap(j).wait_recv()
        dn_load(j).start()
        dn_swap(j).start()
        matmul(blocks(opening, j), j)

    pass_meta(2)
    loop(0, nch, first_chunks)
    activate(opening)

    def gather_step(s):
        def chunk(j):
            pass_on(s, j)
            matmul(blocks((s, n - s), j), j)
        pass_meta(s)
        loop(0, nch, chunk)
        activate((s, n - s))

    loop(3, half - 2, gather_step)

    def send_few(way, last, picked, j):
        few_out[way, j] = jnp.dot(picked, tok[last, j], preferred_element_type=F32).astype(BF16)
        ag_few(way, j).start()

    pass_meta(half - 2)
    edge_back = n - half + 2
    picked_back = pick(edge_back, behind)[:, :rows].astype(BF16)

    def back_edge(j):
        arrive(ag(AHEAD, half - 2, j))
        ag(AHEAD, half - 1, j).start()
        arrive(ag(BEHIND, half - 2, j))
        send_few(BEHIND, edge_back, picked_back, j)
        matmul(blocks((half - 2, edge_back), j), j)

    loop(0, nch, back_edge)
    activate((half - 2, edge_back))

    pass_meta(half - 1, (AHEAD,))
    edge = half - 1
    picked_ahead = pick(edge, ahead)[:, :rows].astype(BF16)

    def ahead_edge(j):
        arrive(ag(AHEAD, edge, j))
        send_few(AHEAD, edge, picked_ahead, j)
        ag_few(BEHIND, j).wait_recv()
        matmul(jnp.concatenate([tok[edge, j], few_in[BEHIND, j]], axis=0), j)

    loop(0, nch, ahead_edge)
    for j in range(nch):
        dn_load(j).wait()
        dn_swap(j).wait_recv()
    activate((edge,), (BEHIND,))

    def return_few(came):
        way = 1 - came

        def body(j):
            back_out[way, j] = jnp.dot(
                hid_few[came], wd[j], preferred_element_type=F32).astype(BF16)
            rs_few(way, j).start()
        loop(0, nch, body)

    return_few(BEHIND)

    def few_chunk(j):
        ag_few(AHEAD, j).wait_recv()
        matmul(few_in[AHEAD, j], j)

    loop(0, nch, few_chunk)
    arrive(ag_meta(AHEAD, half))
    activate((), (AHEAD,))
    return_few(AHEAD)

    def first_sums(came, d, chip):
        way = 1 - came
        a = slot(came, d)
        placed = unpick(a, chip)

        def body(j):
            mine = jnp.dot(hid[a], wd[j], preferred_element_type=F32)
            rs_few(way, j).wait_recv()
            mine += jnp.dot(placed, back_in[way, j], preferred_element_type=F32)
            part[way, d, j] = mine.astype(BF16)
            rs(way, d, j).start()
        loop(0, nch, body)

    first_sums(BEHIND, half - 2, behind)
    first_sums(AHEAD, half - 1, ahead)

    def add_part(way, d, j, own):
        rs(way, d + 1, j).wait_recv()
        part[way, d, j] = (own + part[way, d, j].astype(F32)).astype(BF16)
        rs(way, d + 1, j).wait_send()

    def reduce_step(i):
        d = half - 2 - i

        def chunk(j):
            h = jnp.concatenate([hid[n - d + 1], hid[d]], axis=0)
            mine = jnp.dot(h, wd[j], preferred_element_type=F32)
            add_part(AHEAD, d - 1, j, mine[:rows])
            add_part(BEHIND, d, j, mine[rows:])
            rs(AHEAD, d - 1, j).start()
            rs(BEHIND, d, j).start()
        loop(0, nch, chunk)

    loop(0, half - 3, reduce_step)

    def last_sums(j):
        add_part(BEHIND, 1, j, jnp.dot(hid[1], wd[j], preferred_element_type=F32))
        rs(BEHIND, 1, j).start()

    loop(0, nch, last_sums)

    def out_copy(j):
        return pltpu.make_async_copy(
            out_buf.at[j], out_hbm.at[:, pl.ds(j * width, width)], out_sem.at[j])

    for j in range(nch):
        total = jnp.dot(hid[0], wd[j], preferred_element_type=F32)
        for way in (AHEAD, BEHIND):
            arrive(rs(way, 1, j))
            total = total + part[way, 0, j].astype(F32)
        out_buf[j] = total.astype(BF16)
        out_copy(j).start()
    for j in range(nch):
        gu_swap(j).wait_send()
        dn_swap(j).wait_send()
        for way in (AHEAD, BEHIND):
            ag_few(way, j).wait_send()
            rs_few(way, j).wait_send()
        out_copy(j).wait()


def on_device(n, tokens, expert_ids, gate_weights, gate_up_weight, down_weight):
    rows, model = tokens.shape
    top = expert_ids.shape[1]
    inner = down_weight.shape[1]
    experts = 2 * n
    cap = 2 * rows * top // experts
    few = 2 * cap
    nch = 4
    width = model // nch
    half = n // 2
    dma = pltpu.SemaphoreType.DMA
    hbm = pl.BlockSpec(memory_space=pl.ANY)
    return pl.pallas_call(
        functools.partial(moe_kernel, n, nch, top, cap),
        out_shape=jax.ShapeDtypeStruct((rows, model), BF16),
        in_specs=[hbm] * 5,
        out_specs=hbm,
        scratch_shapes=[
            pltpu.VMEM((n, nch, rows, width), BF16),
            pltpu.VMEM((top, rows), jnp.int32),
            pltpu.VMEM((top, rows), F32),
            pltpu.VMEM((n, top, 128), F32),
            pltpu.VMEM((2, model, 2 * inner), BF16),
            pltpu.VMEM((nch, 2 * inner, width), BF16),
            pltpu.VMEM((n, rows, 2 * inner), BF16),
            pltpu.VMEM((2, few, 2 * inner), BF16),
            pltpu.VMEM((5 * rows, 4 * inner), F32),
            pltpu.VMEM((2, half, nch, rows, width), BF16),
            pltpu.VMEM((nch, rows, width), BF16),
            pltpu.VMEM((2, nch, few, width), BF16),
            pltpu.VMEM((2, nch, few, width), BF16),
            pltpu.VMEM((2, nch, few, width), BF16),
            pltpu.VMEM((2, nch, few, width), BF16),
            dma((3 * nch + 2,)),
            dma((nch,)),
            dma((2 * nch,)),
            dma((2 * nch,)),
            dma((2, nch)),
            dma((2, half, nch)),
            dma((2,)),
            dma((2, half + 1)),
            dma((2, nch)),
            dma((2, nch)),
            dma((2, nch)),
            dma((2, half, nch)),
            dma((2, nch)),
            dma((2, nch)),
        ],
        compiler_params=pltpu.CompilerParams(
            collective_id=0, has_side_effects=True, vmem_limit_bytes=66_000_000),
        name="moe_ring",
    )(tokens, expert_ids.T, gate_weights.T, gate_up_weight, down_weight)


def solution(mesh):
    placed = (
        P(("groups", "ep", "node"), None),
        P(("groups", "ep", "node"), None),
        P(("groups", "ep", "node"), None),
        P(("ep", "node"), None, None),
        P(("ep", "node"), None, None),
    )
    return jax.shard_map(
        functools.partial(on_device, mesh.shape["ep"]),
        mesh=mesh,
        in_specs=placed,
        out_specs=P(("groups", "ep", "node"), None),
        check_vma=False,
    )
```

```python
import functools

import jax
import jax.numpy as jnp
from jax import lax
from jax.experimental import pallas as pl
from jax.experimental.pallas import tpu as pltpu
from jax.sharding import PartitionSpec as P

MESH = pl.DeviceIdType.MESH
BF16 = jnp.bfloat16
F32 = jnp.float32
AHEAD, BEHIND = 0, 1


def moe_kernel(
    n, nch, top, cap,
    tok_hbm, ids_hbm, gates_hbm, gu_hbm, dn_hbm, out_hbm,
    tok, ids_in, gates_in, meta, wgu, wd, hid, hid_few, acc, part, out_buf,
    few_out, few_in, back_out, back_in,
    load_sem, out_sem, w_send, w_recv, ag_send, ag_recv, meta_send, meta_recv,
    few_send, few_recv, rs_send, rs_recv, back_send, back_recv,
):
    half = n // 2
    few = 2 * cap
    rows, width = tok.shape[2], tok.shape[3]
    inner = dn_hbm.shape[1]
    me = lax.axis_index("ep")
    core = lax.axis_index("node")
    peer = 1 - core
    ahead = lax.rem(me + 1 + core * (n - 2), n)
    behind = lax.rem(me + n - 1 - core * (n - 2), n)
    to = (ahead, behind)

    barrier = pltpu.get_barrier_semaphore()
    pl.semaphore_signal(barrier, inc=1, device_id={"ep": ahead}, device_id_type=MESH)
    pl.semaphore_signal(barrier, inc=1, device_id={"ep": behind}, device_id_type=MESH)
    pl.semaphore_signal(barrier, inc=1, device_id={"node": peer}, device_id_type=MESH)

    tok_loads = [pltpu.make_async_copy(
        tok_hbm.at[:, pl.ds(j * width, width)], tok.at[0, j], load_sem.at[j]) for j in range(nch)]
    meta_loads = [
        pltpu.make_async_copy(ids_hbm, ids_in, load_sem.at[nch]),
        pltpu.make_async_copy(gates_hbm, gates_in, load_sem.at[nch + 1]),
    ]
    for c in meta_loads + tok_loads:
        c.start()

    def gu_load(j):
        at = pl.ds(j * width, width)
        return pltpu.make_async_copy(gu_hbm.at[0, at], wgu.at[0, at], load_sem.at[nch + 2 + j])

    def gu_swap(j):
        at = pl.ds(j * width, width)
        return pltpu.make_async_remote_copy(
            src_ref=gu_hbm.at[0, at], dst_ref=wgu.at[1, at],
            send_sem=w_send.at[j], recv_sem=w_recv.at[j],
            device_id={"node": peer}, device_id_type=MESH)

    def dn_load(j):
        return pltpu.make_async_copy(
            dn_hbm.at[0, :, pl.ds(j * width, width)], wd.at[j, pl.ds(0, inner)],
            load_sem.at[2 * nch + 2 + j])

    def dn_swap(j):
        return pltpu.make_async_remote_copy(
            src_ref=dn_hbm.at[0, :, pl.ds(j * width, width)], dst_ref=wd.at[j, pl.ds(inner, inner)],
            send_sem=w_send.at[nch + j], recv_sem=w_recv.at[nch + j],
            device_id={"node": peer}, device_id_type=MESH)

    for c in meta_loads:
        c.wait()
    coarse = gates_in[...].astype(BF16).astype(F32)
    meta[0] = jnp.concatenate(
        [ids_in[...].astype(F32), coarse, gates_in[...] - coarse,
         jnp.zeros((top, 128 - 3 * rows), F32)], axis=1).astype(BF16)
    pl.semaphore_wait(barrier, 3)

    def slot(way, s):
        return s if way == AHEAD else lax.rem(n - s, n)

    def ag(way, s, j):
        return pltpu.make_async_remote_copy(
            src_ref=tok.at[slot(way, s - 1), j], dst_ref=tok.at[slot(way, s), j],
            send_sem=ag_send.at[way, j], recv_sem=ag_recv.at[way, s, j],
            device_id={"ep": to[way]}, device_id_type=MESH)

    def ag_meta(way, s):
        return pltpu.make_async_remote_copy(
            src_ref=meta.at[slot(way, s - 1)], dst_ref=meta.at[slot(way, s)],
            send_sem=meta_send.at[way], recv_sem=meta_recv.at[way, s],
            device_id={"ep": to[way]}, device_id_type=MESH)

    def ag_few(way, j):
        return pltpu.make_async_remote_copy(
            src_ref=few_out.at[way, j], dst_ref=few_in.at[way, j],
            send_sem=few_send.at[way, j], recv_sem=few_recv.at[way, j],
            device_id={"ep": to[way]}, device_id_type=MESH)

    def rs(way, d, j):
        return pltpu.make_async_remote_copy(
            src_ref=part.at[way, d, j], dst_ref=part.at[way, d - 1, j],
            send_sem=rs_send.at[way, j], recv_sem=rs_recv.at[way, d - 1, j],
            device_id={"ep": to[way]}, device_id_type=MESH)

    def rs_few(way, j):
        return pltpu.make_async_remote_copy(
            src_ref=back_out.at[way, j], dst_ref=back_in.at[way, j],
            send_sem=back_send.at[way, j], recv_sem=back_recv.at[way, j],
            device_id={"ep": to[way]}, device_id_type=MESH)

    def loop(lo, hi, body):
        def step(i, carry):
            body(i)
            return carry
        lax.fori_loop(lo, hi, step, 0)

    def matmul(x, j):
        for e in range(2):
            at = pl.ds(e * 2 * inner, 2 * inner)
            w = wgu[e, pl.ds(pl.multiple_of(j * width, width), width), :]
            acc[: x.shape[0], at] += jnp.dot(x, w, preferred_element_type=F32)

    def blocks(slots, j):
        return jnp.concatenate([tok[a, j] for a in slots], axis=0)

    lane = lax.broadcasted_iota(jnp.int32, (rows, 128), 1)
    same = lax.broadcasted_iota(jnp.int32, (rows, 128), 0) == lane
    before = (lax.broadcasted_iota(jnp.int32, (128, 128), 0)
              < lax.broadcasted_iota(jnp.int32, (128, 128), 1)).astype(F32).astype(BF16)

    def expert(chip, e):
        return (chip * 2 + (core if e == 0 else peer)).astype(F32)

    def gate_row(a, name):
        ids = meta[a].astype(F32)
        gates = pltpu.roll(ids, 128 - rows, 1) + pltpu.roll(ids, 128 - 2 * rows, 1)
        return jnp.sum(jnp.where(ids == name, gates, 0.0), axis=0, keepdims=True)

    def chosen_row(a, name):
        return jnp.sum(jnp.where(meta[a].astype(F32) == name, 1.0, 0.0), axis=0, keepdims=True)

    def rank_row(chosen):
        wide = jnp.broadcast_to(chosen, (8, 128)).astype(BF16)
        return jnp.dot(wide, before, preferred_element_type=F32)[0:1]

    def column(row):
        return jnp.sum(jnp.where(same, row, 0.0), axis=1, keepdims=True)

    def pick(a, chip):
        place = lax.broadcasted_iota(jnp.int32, (few, 128), 0).astype(F32)
        found = jnp.zeros((few, 128), F32)
        for e in range(2):
            chosen = chosen_row(a, expert(chip, e))
            found += jnp.where(place - e * cap == rank_row(chosen), chosen, 0.0)
        return found

    def unpick(a, chip):
        place = lane.astype(F32)
        found = jnp.zeros((rows, 128), F32)
        for e in range(2):
            chosen = chosen_row(a, expert(chip, e))
            found += jnp.where(place - e * cap == column(rank_row(chosen)), column(chosen), 0.0)
        return found[:, :few].astype(BF16)

    def gate_all(a, e):
        return column(gate_row(a, expert(me, e)))

    def gate_few(a, e):
        place = lax.broadcasted_iota(jnp.int32, (few, 128), 0).astype(F32) - e * cap
        name = expert(me, e)
        chosen = chosen_row(a, name)
        hit = jnp.where(place == rank_row(chosen), chosen * gate_row(a, name), 0.0)
        return jnp.sum(jnp.where(lax.broadcasted_iota(jnp.int32, (few, 128), 1) < rows, hit, 0.0),
                       axis=1, keepdims=True)

    def activate(slots, few_slots=()):
        count = len(slots) * rows + len(few_slots) * few
        for e in range(2):
            g = jnp.concatenate(
                [gate_all(a, e) for a in slots]
                + [gate_few(slot(way, half - way), e) for way in few_slots], axis=0)
            gate = acc[:count, pl.ds(e * 2 * inner, inner)]
            up = acc[:count, pl.ds(e * 2 * inner + inner, inner)]
            h = (gate * (1.0 / (1.0 + jnp.exp(-gate))) * up * g).astype(BF16)
            at = pl.ds(e * inner, inner)
            for i, a in enumerate(slots):
                hid[a, :, at] = h[i * rows:(i + 1) * rows]
            for i, way in enumerate(few_slots):
                first = len(slots) * rows + i * few
                hid_few[way, :, at] = h[first:first + few]
        acc[:count, :] = jnp.zeros((count, 4 * inner), F32)

    for way in (AHEAD, BEHIND):
        ag_meta(way, 1).start()
    for j in range(nch):
        tok_loads[j].wait()
        for way in (AHEAD, BEHIND):
            ag(way, 1, j).start()
    for j in range(nch):
        gu_load(j).start()
        gu_swap(j).start()
    acc[...] = jnp.zeros_like(acc)

    def arrive(copy):
        copy.wait_recv()
        copy.wait_send()

    def pass_on(s, j):
        for way in (AHEAD, BEHIND):
            arrive(ag(way, s, j))
            ag(way, s + 1, j).start()

    def pass_meta(s, ways=(AHEAD, BEHIND)):
        for way in (AHEAD, BEHIND):
            arrive(ag_meta(way, s))
            if way in ways:
                ag_meta(way, s + 1).start()

    pass_meta(1)
    loop(0, nch, lambda j: pass_on(1, j))

    opening = (0, 1, n - 1, 2, n - 2)

    def first_chunks(j):
        pass_on(2, j)
        gu_load(j).wait()
        gu_swap(j).wait_recv()
        dn_load(j).start()
        dn_swap(j).start()
        matmul(blocks(opening, j), j)

    pass_meta(2)
    loop(0, nch, first_chunks)
    activate(opening)

    def gather_step(s):
        def chunk(j):
            pass_on(s, j)
            matmul(blocks((s, n - s), j), j)
        pass_meta(s)
        loop(0, nch, chunk)
        activate((s, n - s))

    loop(3, half - 2, gather_step)

    def send_few(way, last, picked, j):
        few_out[way, j] = jnp.dot(picked, tok[last, j], preferred_element_type=F32).astype(BF16)
        ag_few(way, j).start()

    pass_meta(half - 2)
    edge_back = n - half + 2
    picked_back = pick(edge_back, behind)[:, :rows].astype(BF16)

    def back_edge(j):
        arrive(ag(AHEAD, half - 2, j))
        ag(AHEAD, half - 1, j).start()
        arrive(ag(BEHIND, half - 2, j))
        send_few(BEHIND, edge_back, picked_back, j)
        matmul(blocks((half - 2, edge_back), j), j)

    loop(0, nch, back_edge)
    activate((half - 2, edge_back))

    pass_meta(half - 1, (AHEAD,))
    edge = half - 1
    picked_ahead = pick(edge, ahead)[:, :rows].astype(BF16)

    def ahead_edge(j):
        arrive(ag(AHEAD, edge, j))
        send_few(AHEAD, edge, picked_ahead, j)
        ag_few(BEHIND, j).wait_recv()
        matmul(jnp.concatenate([tok[edge, j], few_in[BEHIND, j]], axis=0), j)

    loop(0, nch, ahead_edge)
    for j in range(nch):
        dn_load(j).wait()
        dn_swap(j).wait_recv()
    activate((edge,), (BEHIND,))

    def return_few(came):
        way = 1 - came

        def body(j):
            back_out[way, j] = jnp.dot(
                hid_few[came], wd[j], preferred_element_type=F32).astype(BF16)
            rs_few(way, j).start()
        loop(0, nch, body)

    def first_sums(came, d, chip):
        way = 1 - came
        a = slot(came, d)
        placed = unpick(a, chip)

        def body(j):
            mine = jnp.dot(hid[a], wd[j], preferred_element_type=F32)
            rs_few(way, j).wait_recv()
            mine += jnp.dot(placed, back_in[way, j], preferred_element_type=F32)
            part[way, d, j] = mine.astype(BF16)
            rs(way, d, j).start()
        loop(0, nch, body)

    return_few(BEHIND)
    first_sums(BEHIND, half - 2, behind)

    def few_chunk(j):
        ag_few(AHEAD, j).wait_recv()
        matmul(few_in[AHEAD, j], j)

    loop(0, nch, few_chunk)
    arrive(ag_meta(AHEAD, half))
    activate((), (AHEAD,))
    return_few(AHEAD)
    first_sums(AHEAD, half - 1, ahead)

    def add_part(way, d, j, own):
        rs(way, d + 1, j).wait_recv()
        part[way, d, j] = (own + part[way, d, j].astype(F32)).astype(BF16)
        rs(way, d + 1, j).wait_send()

    def reduce_step(i):
        d = half - 2 - i

        def chunk(j):
            h = jnp.concatenate([hid[n - d + 1], hid[d]], axis=0)
            mine = jnp.dot(h, wd[j], preferred_element_type=F32)
            add_part(AHEAD, d - 1, j, mine[:rows])
            add_part(BEHIND, d, j, mine[rows:])
            rs(AHEAD, d - 1, j).start()
            rs(BEHIND, d, j).start()
        loop(0, nch, chunk)

    loop(0, half - 3, reduce_step)

    def last_sums(j):
        add_part(BEHIND, 1, j, jnp.dot(hid[1], wd[j], preferred_element_type=F32))
        rs(BEHIND, 1, j).start()

    loop(0, nch, last_sums)

    def out_copy(j):
        return pltpu.make_async_copy(
            out_buf.at[j], out_hbm.at[:, pl.ds(j * width, width)], out_sem.at[j])

    for j in range(nch):
        total = jnp.dot(hid[0], wd[j], preferred_element_type=F32)
        for way in (AHEAD, BEHIND):
            arrive(rs(way, 1, j))
            total = total + part[way, 0, j].astype(F32)
        out_buf[j] = total.astype(BF16)
        out_copy(j).start()
    for j in range(nch):
        gu_swap(j).wait_send()
        dn_swap(j).wait_send()
        for way in (AHEAD, BEHIND):
            ag_few(way, j).wait_send()
            rs_few(way, j).wait_send()
        out_copy(j).wait()


def on_device(n, tokens, expert_ids, gate_weights, gate_up_weight, down_weight):
    rows, model = tokens.shape
    top = expert_ids.shape[1]
    inner = down_weight.shape[1]
    experts = 2 * n
    cap = 2 * rows * top // experts
    few = 2 * cap
    nch = 4
    width = model // nch
    half = n // 2
    dma = pltpu.SemaphoreType.DMA
    hbm = pl.BlockSpec(memory_space=pl.ANY)
    return pl.pallas_call(
        functools.partial(moe_kernel, n, nch, top, cap),
        out_shape=jax.ShapeDtypeStruct((rows, model), BF16),
        in_specs=[hbm] * 5,
        out_specs=hbm,
        scratch_shapes=[
            pltpu.VMEM((n, nch, rows, width), BF16),
            pltpu.VMEM((top, rows), jnp.int32),
            pltpu.VMEM((top, rows), F32),
            pltpu.VMEM((n, top, 128), BF16),
            pltpu.VMEM((2, model, 2 * inner), BF16),
            pltpu.VMEM((nch, 2 * inner, width), BF16),
            pltpu.VMEM((n, rows, 2 * inner), BF16),
            pltpu.VMEM((2, few, 2 * inner), BF16),
            pltpu.VMEM((5 * rows, 4 * inner), F32),
            pltpu.VMEM((2, half, nch, rows, width), BF16),
            pltpu.VMEM((nch, rows, width), BF16),
            pltpu.VMEM((2, nch, few, width), BF16),
            pltpu.VMEM((2, nch, few, width), BF16),
            pltpu.VMEM((2, nch, few, width), BF16),
            pltpu.VMEM((2, nch, few, width), BF16),
            dma((3 * nch + 2,)),
            dma((nch,)),
            dma((2 * nch,)),
            dma((2 * nch,)),
            dma((2, nch)),
            dma((2, half, nch)),
            dma((2,)),
            dma((2, half + 1)),
            dma((2, nch)),
            dma((2, nch)),
            dma((2, nch)),
            dma((2, half, nch)),
            dma((2, nch)),
            dma((2, nch)),
        ],
        compiler_params=pltpu.CompilerParams(
            collective_id=0, has_side_effects=True, vmem_limit_bytes=66_000_000),
        name="moe_ring",
    )(tokens, expert_ids.T, gate_weights.T, gate_up_weight, down_weight)


def solution(mesh):
    placed = (
        P(("groups", "ep", "node"), None),
        P(("groups", "ep", "node"), None),
        P(("groups", "ep", "node"), None),
        P(("ep", "node"), None, None),
        P(("ep", "node"), None, None),
    )
    return jax.shard_map(
        functools.partial(on_device, mesh.shape["ep"]),
        mesh=mesh,
        in_specs=placed,
        out_specs=P(("groups", "ep", "node"), None),
        check_vma=False,
    )
```

```python
import functools

import jax
import jax.numpy as jnp
from jax import lax
from jax.experimental import pallas as pl
from jax.experimental.pallas import tpu as pltpu
from jax.sharding import PartitionSpec as P

MESH = pl.DeviceIdType.MESH
BF16 = jnp.bfloat16
F32 = jnp.float32
AHEAD, BEHIND = 0, 1


def moe_kernel(
    n, nch, top, cap,
    tok_hbm, ids_hbm, gates_hbm, gu_hbm, dn_hbm, out_hbm,
    tok, ids_in, gates_in, meta, wgu, wd, hid, hid_few, acc, part, out_buf,
    few_out, few_in, back_out, back_in,
    load_sem, out_sem, w_send, w_recv, ag_send, ag_recv, meta_send, meta_recv,
    few_send, few_recv, rs_send, rs_recv, back_send, back_recv,
):
    half = n // 2
    few = 2 * cap
    rows, width = tok.shape[2], tok.shape[3]
    inner = dn_hbm.shape[1]
    me = lax.axis_index("ep")
    core = lax.axis_index("node")
    peer = 1 - core
    ahead = lax.rem(me + 1 + core * (n - 2), n)
    behind = lax.rem(me + n - 1 - core * (n - 2), n)
    to = (ahead, behind)

    barrier = pltpu.get_barrier_semaphore()
    pl.semaphore_signal(barrier, inc=1, device_id={"ep": ahead}, device_id_type=MESH)
    pl.semaphore_signal(barrier, inc=1, device_id={"ep": behind}, device_id_type=MESH)
    pl.semaphore_signal(barrier, inc=1, device_id={"node": peer}, device_id_type=MESH)

    tok_loads = [pltpu.make_async_copy(
        tok_hbm.at[:, pl.ds(j * width, width)], tok.at[0, j], load_sem.at[j]) for j in range(nch)]
    meta_loads = [
        pltpu.make_async_copy(ids_hbm, ids_in, load_sem.at[nch]),
        pltpu.make_async_copy(gates_hbm, gates_in, load_sem.at[nch + 1]),
    ]
    for c in meta_loads + tok_loads:
        c.start()

    def gu_load(j):
        at = pl.ds(j * width, width)
        return pltpu.make_async_copy(gu_hbm.at[0, at], wgu.at[0, at], load_sem.at[nch + 2 + j])

    def gu_swap(j):
        at = pl.ds(j * width, width)
        return pltpu.make_async_remote_copy(
            src_ref=gu_hbm.at[0, at], dst_ref=wgu.at[1, at],
            send_sem=w_send.at[j], recv_sem=w_recv.at[j],
            device_id={"node": peer}, device_id_type=MESH)

    def dn_load(j):
        return pltpu.make_async_copy(
            dn_hbm.at[0, :, pl.ds(j * width, width)], wd.at[j, pl.ds(0, inner)],
            load_sem.at[2 * nch + 2 + j])

    def dn_swap(j):
        return pltpu.make_async_remote_copy(
            src_ref=dn_hbm.at[0, :, pl.ds(j * width, width)], dst_ref=wd.at[j, pl.ds(inner, inner)],
            send_sem=w_send.at[nch + j], recv_sem=w_recv.at[nch + j],
            device_id={"node": peer}, device_id_type=MESH)

    for c in meta_loads:
        c.wait()
    coarse = gates_in[...].astype(BF16).astype(F32)
    meta[0] = jnp.concatenate(
        [ids_in[...].astype(F32), coarse, gates_in[...] - coarse,
         jnp.zeros((top, 128 - 3 * rows), F32)], axis=1).astype(BF16)
    pl.semaphore_wait(barrier, 3)

    def slot(way, s):
        return s if way == AHEAD else lax.rem(n - s, n)

    def ag(way, s, j):
        return pltpu.make_async_remote_copy(
            src_ref=tok.at[slot(way, s - 1), j], dst_ref=tok.at[slot(way, s), j],
            send_sem=ag_send.at[way, j], recv_sem=ag_recv.at[way, s, j],
            device_id={"ep": to[way]}, device_id_type=MESH)

    def ag_meta(way, s):
        return pltpu.make_async_remote_copy(
            src_ref=meta.at[slot(way, s - 1)], dst_ref=meta.at[slot(way, s)],
            send_sem=meta_send.at[way], recv_sem=meta_recv.at[way, s],
            device_id={"ep": to[way]}, device_id_type=MESH)

    def ag_few(way, j):
        return pltpu.make_async_remote_copy(
            src_ref=few_out.at[way, j], dst_ref=few_in.at[way, j],
            send_sem=few_send.at[way, j], recv_sem=few_recv.at[way, j],
            device_id={"ep": to[way]}, device_id_type=MESH)

    def rs(way, d, j):
        return pltpu.make_async_remote_copy(
            src_ref=part.at[way, d, j], dst_ref=part.at[way, d - 1, j],
            send_sem=rs_send.at[way, j], recv_sem=rs_recv.at[way, d - 1, j],
            device_id={"ep": to[way]}, device_id_type=MESH)

    def rs_few(way, j):
        return pltpu.make_async_remote_copy(
            src_ref=back_out.at[way, j], dst_ref=back_in.at[way, j],
            send_sem=back_send.at[way, j], recv_sem=back_recv.at[way, j],
            device_id={"ep": to[way]}, device_id_type=MESH)

    def loop(lo, hi, body):
        def step(i, carry):
            body(i)
            return carry
        lax.fori_loop(lo, hi, step, 0)

    def matmul(x, j):
        for e in range(2):
            at = pl.ds(e * 2 * inner, 2 * inner)
            w = wgu[e, pl.ds(pl.multiple_of(j * width, width), width), :]
            acc[: x.shape[0], at] += jnp.dot(x, w, preferred_element_type=F32)

    def blocks(slots, j):
        return jnp.concatenate([tok[a, j] for a in slots], axis=0)

    lane = lax.broadcasted_iota(jnp.int32, (rows, 128), 1)
    same = lax.broadcasted_iota(jnp.int32, (rows, 128), 0) == lane
    before = (lax.broadcasted_iota(jnp.int32, (128, 128), 0)
              < lax.broadcasted_iota(jnp.int32, (128, 128), 1)).astype(F32).astype(BF16)

    def expert(chip, e):
        return (chip * 2 + (core if e == 0 else peer)).astype(F32)

    def gate_row(a, name):
        ids = meta[a].astype(F32)
        gates = pltpu.roll(ids, 128 - rows, 1) + pltpu.roll(ids, 128 - 2 * rows, 1)
        return jnp.sum(jnp.where(ids == name, gates, 0.0), axis=0, keepdims=True)

    def chosen_row(a, name):
        return jnp.sum(jnp.where(meta[a].astype(F32) == name, 1.0, 0.0), axis=0, keepdims=True)

    def rank_row(chosen):
        wide = jnp.broadcast_to(chosen, (8, 128)).astype(BF16)
        return jnp.dot(wide, before, preferred_element_type=F32)[0:1]

    def column(row):
        return jnp.sum(jnp.where(same, row, 0.0), axis=1, keepdims=True)

    def pick(a, chip):
        place = lax.broadcasted_iota(jnp.int32, (few, 128), 0).astype(F32)
        found = jnp.zeros((few, 128), F32)
        for e in range(2):
            chosen = chosen_row(a, expert(chip, e))
            found += jnp.where(place - e * cap == rank_row(chosen), chosen, 0.0)
        return found

    def unpick(a, chip):
        place = lane.astype(F32)
        found = jnp.zeros((rows, 128), F32)
        for e in range(2):
            chosen = chosen_row(a, expert(chip, e))
            found += jnp.where(place - e * cap == column(rank_row(chosen)), column(chosen), 0.0)
        return found[:, :few].astype(BF16)

    def gate_all(a, e):
        return column(gate_row(a, expert(me, e)))

    def gate_few(a, e):
        place = lax.broadcasted_iota(jnp.int32, (few, 128), 0).astype(F32) - e * cap
        name = expert(me, e)
        chosen = chosen_row(a, name)
        hit = jnp.where(place == rank_row(chosen), chosen * gate_row(a, name), 0.0)
        return jnp.sum(jnp.where(lax.broadcasted_iota(jnp.int32, (few, 128), 1) < rows, hit, 0.0),
                       axis=1, keepdims=True)

    def activate(slots, few_slots=()):
        count = len(slots) * rows + len(few_slots) * few
        for e in range(2):
            g = jnp.concatenate(
                [gate_all(a, e) for a in slots]
                + [gate_few(slot(way, half - way), e) for way in few_slots], axis=0)
            gate = acc[:count, pl.ds(e * 2 * inner, inner)]
            up = acc[:count, pl.ds(e * 2 * inner + inner, inner)]
            h = (gate * (1.0 / (1.0 + jnp.exp(-gate))) * up * g).astype(BF16)
            at = pl.ds(e * inner, inner)
            for i, a in enumerate(slots):
                hid[a, :, at] = h[i * rows:(i + 1) * rows]
            for i, way in enumerate(few_slots):
                first = len(slots) * rows + i * few
                hid_few[way, :, at] = h[first:first + few]
        acc[:count, :] = jnp.zeros((count, 4 * inner), F32)

    for way in (AHEAD, BEHIND):
        ag_meta(way, 1).start()
    for j in range(nch):
        tok_loads[j].wait()
        for way in (AHEAD, BEHIND):
            ag(way, 1, j).start()
    for j in range(nch):
        gu_load(j).start()
        gu_swap(j).start()
    acc[...] = jnp.zeros_like(acc)

    def arrive(copy):
        copy.wait_recv()
        copy.wait_send()

    def pass_on(s, j):
        for way in (AHEAD, BEHIND):
            arrive(ag(way, s, j))
            ag(way, s + 1, j).start()

    def pass_meta(s, ways=(AHEAD, BEHIND)):
        for way in (AHEAD, BEHIND):
            arrive(ag_meta(way, s))
            if way in ways:
                ag_meta(way, s + 1).start()

    pass_meta(1)
    loop(0, nch, lambda j: pass_on(1, j))

    opening = (0, 1, n - 1, 2, n - 2)

    def first_chunks(j):
        pass_on(2, j)
        gu_load(j).wait()
        gu_swap(j).wait_recv()
        dn_load(j).start()
        dn_swap(j).start()
        matmul(blocks(opening, j), j)

    pass_meta(2)
    loop(0, nch, first_chunks)
    activate(opening)

    def gather_step(s):
        def chunk(j):
            pass_on(s, j)
            matmul(blocks((s, n - s), j), j)
        pass_meta(s)
        loop(0, nch, chunk)
        activate((s, n - s))

    loop(3, half - 2, gather_step)

    def send_few(way, last, picked, j):
        few_out[way, j] = jnp.dot(picked, tok[last, j], preferred_element_type=F32).astype(BF16)
        ag_few(way, j).start()

    pass_meta(half - 2)
    edge_back = n - half + 2
    picked_back = pick(edge_back, behind)[:, :rows].astype(BF16)

    def back_edge(j):
        arrive(ag(AHEAD, half - 2, j))
        ag(AHEAD, half - 1, j).start()
        arrive(ag(BEHIND, half - 2, j))
        send_few(BEHIND, edge_back, picked_back, j)
        matmul(blocks((half - 2, edge_back), j), j)

    loop(0, nch, back_edge)
    activate((half - 2, edge_back))

    pass_meta(half - 1, (AHEAD,))
    edge = half - 1
    picked_ahead = pick(edge, ahead)[:, :rows].astype(BF16)
    placed = (unpick(edge, ahead), unpick(edge_back, behind))

    def ahead_edge(j):
        arrive(ag(AHEAD, edge, j))
        send_few(AHEAD, edge, picked_ahead, j)
        ag_few(BEHIND, j).wait_recv()
        matmul(jnp.concatenate([tok[edge, j], few_in[BEHIND, j]], axis=0), j)

    loop(0, nch, ahead_edge)
    for j in range(nch):
        dn_load(j).wait()
        dn_swap(j).wait_recv()
    activate((edge,), (BEHIND,))

    def return_few(came):
        way = 1 - came

        def body(j):
            back_out[way, j] = jnp.dot(
                hid_few[came], wd[j], preferred_element_type=F32).astype(BF16)
            rs_few(way, j).start()
        loop(0, nch, body)

    def first_sums(came, d):
        way = 1 - came
        a = slot(came, d)

        def body(j):
            mine = jnp.dot(hid[a], wd[j], preferred_element_type=F32)
            rs_few(way, j).wait_recv()
            mine += jnp.dot(placed[came], back_in[way, j], preferred_element_type=F32)
            part[way, d, j] = mine.astype(BF16)
            rs(way, d, j).start()
        loop(0, nch, body)

    return_few(BEHIND)

    def few_chunk(j):
        ag_few(AHEAD, j).wait_recv()
        matmul(few_in[AHEAD, j], j)

    loop(0, nch, few_chunk)
    arrive(ag_meta(AHEAD, half))
    activate((), (AHEAD,))
    return_few(AHEAD)
    first_sums(BEHIND, half - 2)
    first_sums(AHEAD, half - 1)

    def add_part(way, d, j, own):
        rs(way, d + 1, j).wait_recv()
        part[way, d, j] = (own + part[way, d, j].astype(F32)).astype(BF16)
        rs(way, d + 1, j).wait_send()

    def reduce_step(i):
        d = half - 2 - i

        def chunk(j):
            h = jnp.concatenate([hid[n - d + 1], hid[d]], axis=0)
            mine = jnp.dot(h, wd[j], preferred_element_type=F32)
            add_part(AHEAD, d - 1, j, mine[:rows])
            add_part(BEHIND, d, j, mine[rows:])
            rs(AHEAD, d - 1, j).start()
            rs(BEHIND, d, j).start()
        loop(0, nch, chunk)

    loop(0, half - 3, reduce_step)

    def last_sums(j):
        add_part(BEHIND, 1, j, jnp.dot(hid[1], wd[j], preferred_element_type=F32))
        rs(BEHIND, 1, j).start()

    loop(0, nch, last_sums)

    def out_copy(j):
        return pltpu.make_async_copy(
            out_buf.at[j], out_hbm.at[:, pl.ds(j * width, width)], out_sem.at[j])

    for j in range(nch):
        total = jnp.dot(hid[0], wd[j], preferred_element_type=F32)
        for way in (AHEAD, BEHIND):
            arrive(rs(way, 1, j))
            total = total + part[way, 0, j].astype(F32)
        out_buf[j] = total.astype(BF16)
        out_copy(j).start()
    for j in range(nch):
        gu_swap(j).wait_send()
        dn_swap(j).wait_send()
        for way in (AHEAD, BEHIND):
            ag_few(way, j).wait_send()
            rs_few(way, j).wait_send()
        out_copy(j).wait()


def on_device(n, tokens, expert_ids, gate_weights, gate_up_weight, down_weight):
    rows, model = tokens.shape
    top = expert_ids.shape[1]
    inner = down_weight.shape[1]
    experts = 2 * n
    cap = 2 * rows * top // experts
    few = 2 * cap
    nch = 4
    width = model // nch
    half = n // 2
    dma = pltpu.SemaphoreType.DMA
    hbm = pl.BlockSpec(memory_space=pl.ANY)
    return pl.pallas_call(
        functools.partial(moe_kernel, n, nch, top, cap),
        out_shape=jax.ShapeDtypeStruct((rows, model), BF16),
        in_specs=[hbm] * 5,
        out_specs=hbm,
        scratch_shapes=[
            pltpu.VMEM((n, nch, rows, width), BF16),
            pltpu.VMEM((top, rows), jnp.int32),
            pltpu.VMEM((top, rows), F32),
            pltpu.VMEM((n, top, 128), BF16),
            pltpu.VMEM((2, model, 2 * inner), BF16),
            pltpu.VMEM((nch, 2 * inner, width), BF16),
            pltpu.VMEM((n, rows, 2 * inner), BF16),
            pltpu.VMEM((2, few, 2 * inner), BF16),
            pltpu.VMEM((5 * rows, 4 * inner), F32),
            pltpu.VMEM((2, half, nch, rows, width), BF16),
            pltpu.VMEM((nch, rows, width), BF16),
            pltpu.VMEM((2, nch, few, width), BF16),
            pltpu.VMEM((2, nch, few, width), BF16),
            pltpu.VMEM((2, nch, few, width), BF16),
            pltpu.VMEM((2, nch, few, width), BF16),
            dma((3 * nch + 2,)),
            dma((nch,)),
            dma((2 * nch,)),
            dma((2 * nch,)),
            dma((2, nch)),
            dma((2, half, nch)),
            dma((2,)),
            dma((2, half + 1)),
            dma((2, nch)),
            dma((2, nch)),
            dma((2, nch)),
            dma((2, half, nch)),
            dma((2, nch)),
            dma((2, nch)),
        ],
        compiler_params=pltpu.CompilerParams(
            collective_id=0, has_side_effects=True, vmem_limit_bytes=66_000_000),
        name="moe_ring",
    )(tokens, expert_ids.T, gate_weights.T, gate_up_weight, down_weight)


def solution(mesh):
    placed = (
        P(("groups", "ep", "node"), None),
        P(("groups", "ep", "node"), None),
        P(("groups", "ep", "node"), None),
        P(("ep", "node"), None, None),
        P(("ep", "node"), None, None),
    )
    return jax.shard_map(
        functools.partial(on_device, mesh.shape["ep"]),
        mesh=mesh,
        in_specs=placed,
        out_specs=P(("groups", "ep", "node"), None),
        check_vma=False,
    )
```
